32 devices in a mesh: rep: 2 (over x), ep: 16 (over z, y, core).
Axes of the slice: x: 2, y: 2, z: 4, core: 2. Of those that a mesh axis runs over, the one named last changes fastest.
Arguments:
- forward_tokens: bfloat16 [2048, 1024], P(('rep', 'ep')), parts along dimension 0, may hold values from -6 to 6
- forward_ids: int32 [2048, 6], P(('rep', 'ep')), parts along dimension 0, may hold values from 0 to 15, all different within a row; in each aligned block of 64 rows (0 to 63, 64 to 127, ...) at most 32 rows name the same one
- forward_mix: float32 [2048, 6], P(('rep', 'ep')), parts along dimension 0, may hold values from 0.1 to 1
- backward_tokens: bfloat16 [2048, 1024], P(('rep', 'ep')), parts along dimension 0, may hold values from -6 to 6
- backward_ids: int32 [2048, 6], P(('rep', 'ep')), parts along dimension 0, may hold values from 0 to 15, all different within a row; in each aligned block of 64 rows (0 to 63, 64 to 127, ...) at most 32 rows name the same one
- backward_mix: float32 [2048, 6], P(('rep', 'ep')), parts along dimension 0, may hold values from 0.1 to 1
- backward_grad: bfloat16 [2048, 1024], P(('rep', 'ep')), parts along dimension 0, may hold values from -6 to 6
- gate_weight: bfloat16 [32, 1024, 704], P(('rep', 'ep')), parts along dimension 0, may hold values from -0.1875 to 0.1875
- up_weight: bfloat16 [32, 1024, 704], P(('rep', 'ep')), parts along dimension 0, may hold values from -0.1875 to 0.1875
- down_weight: bfloat16 [32, 704, 1024], P(('rep', 'ep')), parts along dimension 0, may hold values from -0.21875 to 0.21875
Outputs:
- forward_out: bfloat16 [2048, 1024], P(('rep', 'ep')), parts along dimension 0
- input_grad: bfloat16 [2048, 1024], P(('rep', 'ep')), parts along dimension 0
The draws below stay inside these ranges and needn't reach their ends.
There are 2 independent parts, one for each index of `rep`. The reference program is written for one: setup_inputs(seed, part) draws one part's arguments, and reference() takes and returns one part's arrays. A program takes and returns all parts, laid end to end along the dimension named above; each array names one. Nothing has to cross between parts.
Inputs may be any that keep to these rules, and one draw needn't show every extreme that they name: `forward_ids`: each row names 6 different experts. `forward_ids`: among the 64 rows of one token owner no expert is named more than 32 times, a bound that some block reaches. `backward_ids`: each row names 6 different experts. `backward_ids`: among the 64 rows of one token owner no expert is named more than 32 times, a bound that some block reaches.
All inputs are finite; a program needn't handle non-finite values.
Results may differ from the reference program's by a relative error of at most 0.0058.
Values may be sent and summed in bfloat16 or wider, within the bound.
A program may use at most 64 MiB of HBM per device.

```python
import math
import jax
import jax.numpy as jnp
import numpy as np
from jax import lax

D = 1024
H = 704
TOPK = 6
TOK_DEV = 64
EXPERTS = 16
CAP = 32
TOKENS = 1024
N_EP = 16


def level_of(key, extent, split, smallest, top_value):
    def one(axis_at, shards_of):
        draws = jax.random.uniform(jax.random.fold_in(jax.random.fold_in(key, 6), axis_at), (shards_of,), jnp.float32, smallest / len(split), top_value / len(split))
        return jnp.repeat(jnp.exp(draws), extent[axis_at] // shards_of).reshape((-1,) + (1,) * (len(extent) - axis_at - 1))

    factor_of = one(*split[0])
    for cut in split[1:]:
        factor_of = factor_of * one(*cut)
    return factor_of


def deal_out(stream_key, own, number, rows, number_of, top, reach, skew):
    order = jax.random.permutation(stream_key, number_of)
    crowded, usual = load_shares(number_of, rows * top, reach, skew, True), load_shares(number_of, rows * top, reach, skew, False)
    places = jnp.arange(number_of)

    def named(sizes, offset_by):
        used = int((sizes > 0).sum())
        fixed = max(1, used // 4)
        shifted = fixed + (places - fixed + offset_by * (used - fixed)) % max(1, number_of - fixed)
        return jnp.zeros((number_of,), jnp.int32).at[order[jnp.where(places < fixed, places, shifted)]].set(jnp.asarray(sizes, jnp.int32))

    sizes = jnp.where(number % 4 == 0, named(crowded, number // 4), named(usual, number - number // 4 - 1))
    mixed = jax.random.permutation(jax.random.fold_in(own, 3), number_of)
    donor, sink = mixed[0:number_of // 2 * 2:2], mixed[1:number_of // 2 * 2:2]
    margin = jnp.minimum(sizes[donor] - 1, reach - sizes[sink]) // 2
    margin = jnp.where((donor == order[0]) | (sink == order[0]) | (sizes[sink] == 0), 0, jnp.maximum(margin, 0))
    shifted = jax.random.randint(jax.random.fold_in(own, 4), (number_of // 2,), 0, 1 << 20) % (margin + 1)
    sizes = sizes.at[donor].add(-shifted).at[sink].add(shifted)
    labels = jnp.searchsorted(jnp.cumsum(sizes), jnp.arange(rows * top), side="right").astype(jnp.int32)
    listing = labels.reshape(top, rows).T
    listing = listing[jax.random.permutation(jax.random.fold_in(own, 1), rows)]
    offset_by = jax.random.randint(jax.random.fold_in(own, 2), (rows, 1), 0, top)
    return jnp.take_along_axis(listing, (jnp.arange(top)[None, :] + offset_by) % top, axis=1)


def load_shares(amount, total, limit, slope, full):
    weights = [(1 << 20) // math.isqrt(grade ** slope) + 1 for grade in range(1, amount + 1)]
    largest = limit if full else min(limit, max(-(-total // amount), total * weights[0] // sum(weights)))
    least = 1 if total - largest >= amount - 1 else 0
    given, surplus = [largest] + [least] * (amount - 1), total - largest - least * (amount - 1)
    while surplus > 0:
        free = [i for i in range(1, amount) if given[i] < largest] or [i for i in range(1, amount) if given[i] < limit]
        mass, budget = sum([weights[i] for i in free]), surplus
        for i in free:
            more = min(limit - given[i], max(1, budget * weights[i] // mass), surplus)
            given[i] = given[i] + more
            surplus = surplus - more
    return np.array(given)


def centred(stream_key, shape, scale, most, cuts=(), held_as=jnp.bfloat16):
    array = jax.random.normal(stream_key, shape, jnp.float32) * scale
    if len(cuts) > 0:
        array = level_of(stream_key, shape, cuts, -0.22, 0.18) * array
    return jnp.clip(array, min=-most, max=most).astype(held_as)


def setup_inputs(seed: int = 0, part: int = 0) -> dict:
    key_list = jax.random.split(jax.random.key(seed), 11)
    part_keys = jax.random.split(jax.random.fold_in(key_list[10], part), 11)
    forward_tokens = centred(part_keys[0], (TOKENS, D), 1.0, 6.0, ((0, 16),))
    forward_ids_keys = jax.random.split(jax.random.fold_in(part_keys[1], 1), TOKENS // TOK_DEV)
    forward_ids_turns = jax.random.permutation(jax.random.fold_in(part_keys[1], 3), TOKENS // TOK_DEV)
    forward_ids = jax.vmap(lambda own, number: deal_out(jax.random.fold_in(part_keys[1], 2), own, number, TOK_DEV, EXPERTS, TOPK, CAP, 2))(forward_ids_keys, forward_ids_turns).reshape((TOKENS, TOPK))
    forward_mix = jnp.clip(jnp.exp(math.log(1.0) - 2.3025851 * jax.random.uniform(part_keys[2], (TOKENS, TOPK), jnp.float32) ** level_of(part_keys[2], (TOKENS, TOPK), ((0, 16),), -0.2, 0.2)), 0.1, 1.0)
    backward_tokens = centred(part_keys[3], (TOKENS, D), 1.0, 6.0, ((0, 16),))
    backward_ids_keys = jax.random.split(jax.random.fold_in(part_keys[4], 1), TOKENS // TOK_DEV)
    backward_ids_turns = jax.random.permutation(jax.random.fold_in(part_keys[4], 3), TOKENS // TOK_DEV)
    backward_ids = jax.vmap(lambda own, number: deal_out(jax.random.fold_in(part_keys[4], 2), own, number, TOK_DEV, EXPERTS, TOPK, CAP, 2))(backward_ids_keys, backward_ids_turns).reshape((TOKENS, TOPK))
    backward_mix = jnp.clip(jnp.exp(math.log(1.0) - 2.3025851 * jax.random.uniform(part_keys[5], (TOKENS, TOPK), jnp.float32) ** level_of(part_keys[5], (TOKENS, TOPK), ((0, 16),), -0.2, 0.2)), 0.1, 1.0)
    backward_grad = centred(part_keys[6], (TOKENS, D), 1.0, 6.0, ((0, 16),))
    gate_weight = centred(part_keys[7], (EXPERTS, D, H), D ** -0.5, 0.1875, ((0, 16),))
    up_weight = centred(part_keys[8], (EXPERTS, D, H), D ** -0.5, 0.1875, ((0, 16),))
    down_weight = centred(part_keys[9], (EXPERTS, H, D), H ** -0.5, 0.21875, ((0, 16),))
    return dict(forward_tokens=forward_tokens, forward_ids=forward_ids, forward_mix=forward_mix, backward_tokens=backward_tokens, backward_ids=backward_ids, backward_mix=backward_mix, backward_grad=backward_grad, gate_weight=gate_weight, up_weight=up_weight, down_weight=down_weight)


def expert_forward(expert_rows, gate_matrix, up_matrix, down_matrix):
    gate_pre = jnp.dot(expert_rows, gate_matrix, preferred_element_type=jnp.float32)
    up_pre = jnp.dot(expert_rows, up_matrix, preferred_element_type=jnp.float32)
    hidden = (gate_pre * jax.nn.sigmoid(gate_pre) * up_pre).astype(jnp.bfloat16)
    return jnp.dot(hidden, down_matrix, preferred_element_type=jnp.float32).astype(jnp.bfloat16)


def expert_backward(expert_rows, row_grads, gate_matrix, up_matrix, down_matrix):
    gate_pre = jnp.dot(expert_rows, gate_matrix, preferred_element_type=jnp.float32)
    up_pre = jnp.dot(expert_rows, up_matrix, preferred_element_type=jnp.float32)
    sigmoid_gate = jax.nn.sigmoid(gate_pre)
    hidden_grad = jnp.dot(row_grads, down_matrix.T, preferred_element_type=jnp.float32)
    gate_grad = (hidden_grad * up_pre * sigmoid_gate * (1.0 + gate_pre * (1.0 - sigmoid_gate))).astype(jnp.bfloat16)
    up_grad = (hidden_grad * gate_pre * sigmoid_gate).astype(jnp.bfloat16)
    rows_grad = jnp.dot(gate_grad, gate_matrix.T, preferred_element_type=jnp.float32)
    rows_grad = rows_grad + jnp.dot(up_grad, up_matrix.T, preferred_element_type=jnp.float32)
    return rows_grad.astype(jnp.bfloat16)


def expert_places(expert_ids):
    owners = expert_ids.shape[0] // TOK_DEV
    flat_ids = expert_ids.reshape(owners, TOK_DEV * TOPK)
    onehot = (flat_ids[:, :, None] == jnp.arange(EXPERTS, dtype=jnp.int32)[None, None, :]).astype(jnp.int32)
    before = jnp.cumsum(onehot, axis=1) - onehot
    slot_index = jnp.sum(before * onehot, axis=2).reshape(expert_ids.shape)
    owner_index = (jnp.arange(expert_ids.shape[0], dtype=jnp.int32) // TOK_DEV)[:, None]
    return (owner_index * CAP + slot_index).astype(jnp.int32)


def fill_buffers(values, expert_ids, places):
    spread = jnp.broadcast_to(values[:, None, :], (values.shape[0], TOPK, values.shape[1]))
    empty = jnp.zeros((EXPERTS, N_EP * CAP, values.shape[1]), values.dtype)
    return empty.at[expert_ids, places].set(spread)


def combine(outputs, expert_ids, places, mixing):
    picked = outputs[expert_ids, places].astype(jnp.float32)
    return jnp.sum(mixing[:, :, None] * picked, axis=1).astype(jnp.bfloat16)


def reference(forward_tokens, forward_ids, forward_mix, backward_tokens, backward_ids, backward_mix, backward_grad, gate_weight, up_weight, down_weight):
    places_forward = expert_places(forward_ids)
    buffers = fill_buffers(forward_tokens, forward_ids, places_forward)
    outputs = lax.map(lambda packed: expert_forward(*packed), (buffers, gate_weight, up_weight, down_weight))
    forward_out = combine(outputs, forward_ids, places_forward, forward_mix)
    places_backward = expert_places(backward_ids)
    rows_in = fill_buffers(backward_tokens, backward_ids, places_backward)
    grads_in = fill_buffers(backward_grad, backward_ids, places_backward)
    grads_out = lax.map(lambda packed: expert_backward(*packed), (rows_in, grads_in, gate_weight, up_weight, down_weight))
    input_grad = combine(grads_out, backward_ids, places_backward, backward_mix)
    return (forward_out, input_grad)
```

```python
import functools

import jax
import jax.numpy as jnp
from jax import lax
from jax.experimental import pallas as pl
from jax.experimental.pallas import tpu as pltpu
from jax.sharding import PartitionSpec as P


def expert_forward(expert_rows, gate_matrix, up_matrix, down_matrix):
    gate_pre = jnp.dot(expert_rows, gate_matrix, preferred_element_type=jnp.float32)
    up_pre = jnp.dot(expert_rows, up_matrix, preferred_element_type=jnp.float32)
    hidden = (gate_pre * jax.nn.sigmoid(gate_pre) * up_pre).astype(jnp.bfloat16)
    return jnp.dot(hidden, down_matrix, preferred_element_type=jnp.float32).astype(jnp.bfloat16)


def expert_backward(expert_rows, row_grads, gate_matrix, up_matrix, down_matrix):
    gate_pre = jnp.dot(expert_rows, gate_matrix, preferred_element_type=jnp.float32)
    up_pre = jnp.dot(expert_rows, up_matrix, preferred_element_type=jnp.float32)
    sigmoid_gate = jax.nn.sigmoid(gate_pre)
    hidden_grad = jnp.dot(row_grads, down_matrix.T, preferred_element_type=jnp.float32)
    gate_grad = (
        hidden_grad * up_pre * sigmoid_gate * (1.0 + gate_pre * (1.0 - sigmoid_gate))
    ).astype(jnp.bfloat16)
    up_grad = (hidden_grad * gate_pre * sigmoid_gate).astype(jnp.bfloat16)
    rows_grad = jnp.dot(gate_grad, gate_matrix.T, preferred_element_type=jnp.float32)
    rows_grad = rows_grad + jnp.dot(up_grad, up_matrix.T, preferred_element_type=jnp.float32)
    return rows_grad.astype(jnp.bfloat16)


def route_targets(expert_ids, experts, capacity):
    tok_rows, chosen = expert_ids.shape
    flat_ids = expert_ids.reshape(tok_rows * chosen)
    onehot = (flat_ids[:, None] == jnp.arange(experts, dtype=jnp.int32)[None, :]).astype(jnp.int32)
    before = jnp.cumsum(onehot, axis=0) - onehot
    slot_index = jnp.sum(before * onehot, axis=1)
    return (flat_ids * capacity + slot_index).reshape(tok_rows, chosen)


def dispatch_rows(targets, experts, capacity, sources):
    places = jnp.arange(experts * capacity, dtype=jnp.int32)
    picker = jnp.any(targets[None, :, :] == places[:, None, None], axis=2).astype(jnp.bfloat16)
    return tuple(
        (
            jnp.dot(picker, values, preferred_element_type=jnp.float32)
            .astype(jnp.bfloat16)
            .reshape(experts, capacity, values.shape[1])
            for values in sources
        )
    )


def combine_rows(returned, targets, mixing):
    flat_rows = returned.reshape(returned.shape[0] * returned.shape[1], returned.shape[2])
    picked = flat_rows[targets].astype(jnp.float32)
    return jnp.sum(mixing[:, :, None] * picked, axis=1).astype(jnp.bfloat16)


def run_experts(received, apply, gate_weight, up_weight, down_weight):
    senders = lax.axis_size("ep")
    local_count = gate_weight.shape[0]
    slot_count = received[0].shape[1]
    feature_width = received[0].shape[2]
    expert_rows = tuple(
        (
            values.reshape(senders, local_count, slot_count, feature_width)[:, 0].reshape(
                senders * slot_count, feature_width
            )
            for values in received
        )
    )
    result = apply(expert_rows, gate_weight[0], up_weight[0], down_weight[0])
    outputs = [result.reshape(senders, slot_count, feature_width)]
    return jnp.stack(outputs, axis=1).reshape(senders * local_count, slot_count, feature_width)


def apply_forward(expert_rows, gate_matrix, up_matrix, down_matrix):
    return expert_forward(expert_rows[0], gate_matrix, up_matrix, down_matrix)


def apply_backward(expert_rows, gate_matrix, up_matrix, down_matrix):
    return expert_backward(expert_rows[0], expert_rows[1], gate_matrix, up_matrix, down_matrix)


def per_device(
    forward_tokens,
    forward_ids,
    forward_mix,
    backward_tokens,
    backward_ids,
    backward_mix,
    backward_grad,
    gate_weight,
    up_weight,
    down_weight,
):
    tok_rows, chosen = forward_ids.shape
    experts = lax.axis_size("ep") * gate_weight.shape[0]
    capacity = tok_rows * chosen * 4 // (3 * experts)
    targets_forward = route_targets(forward_ids, experts, capacity)
    targets_backward = route_targets(backward_ids, experts, capacity)
    (sent_forward,) = dispatch_rows(targets_forward, experts, capacity, (forward_tokens,))
    sent_backward, sent_grads = dispatch_rows(
        targets_backward, experts, capacity, (backward_tokens, backward_grad)
    )
    outputs_forward = run_experts(
        (lax.all_to_all(sent_forward, "ep", split_axis=0, concat_axis=0, tiled=True),),
        apply_forward,
        gate_weight,
        up_weight,
        down_weight,
    )
    back_forward = lax.all_to_all(outputs_forward, "ep", split_axis=0, concat_axis=0, tiled=True)
    outputs_backward = run_experts(
        (
            lax.all_to_all(sent_backward, "ep", split_axis=0, concat_axis=0, tiled=True),
            lax.all_to_all(sent_grads, "ep", split_axis=0, concat_axis=0, tiled=True),
        ),
        apply_backward,
        gate_weight,
        up_weight,
        down_weight,
    )
    back_backward = lax.all_to_all(outputs_backward, "ep", split_axis=0, concat_axis=0, tiled=True)
    forward_out = combine_rows(back_forward, targets_forward, forward_mix)
    input_grad = combine_rows(back_backward, targets_backward, backward_mix)
    return (forward_out, input_grad)


MESH_ID = pl.DeviceIdType.MESH
RIGHT, LEFT = 0, 1
TOK_B, GRAD_B, TOK_F, ROUTE = 0, 1, 2, 3
FWD, BWD = 0, 1


def fused_kernel(
    ep,
    cap,
    ft_ref,
    bt_ref,
    bg_ref,
    rt_ref,
    gate_hbm,
    up_hbm,
    down_hbm,
    of_ref,
    ob_ref,
    bt_all,
    bg_all,
    ft_all,
    rt_all,
    gate,
    up,
    down,
    pick,
    mixrow,
    xrows,
    grows,
    zrows,
    pstage,
    precv,
    rstage,
    rrecv,
    wsem,
    ag_send,
    ag_recv,
    dd_send,
    dd_recv,
    ps_send,
    ps_recv,
    rs_send,
    rs_recv,
):
    tok, width = ft_ref.shape
    half = tok // 2
    ring = ep // 2
    arm = ring // 2
    me = lax.axis_index("ep")
    core = lax.rem(me, 2)
    quo = me // 2
    row, col = quo // 2, lax.rem(quo, 2)
    pos = row + col * (ring - 1 - 2 * row)
    partner = me + 1 - 2 * core

    def member(offset, which):
        place = lax.rem(pos + offset + ring, ring)
        side = place // arm
        level = place + side * (ring - 1 - 2 * place)
        return 2 * (2 * level + side) + which

    hop = (member(1, core), member(-1, core))
    sources = (bt_ref, bg_ref, ft_ref, rt_ref)
    gathered = (bt_all, bg_all, ft_all, rt_all)
    started = []

    def remote(src, dst, send, recv, device):
        return pltpu.make_async_remote_copy(
            src_ref=src, dst_ref=dst, send_sem=send, recv_sem=recv,
            device_id={"ep": device}, device_id_type=MESH_ID,
        )

    def launch(copy):
        copy.start()
        started.append(copy)

    barrier = pltpu.get_barrier_semaphore()
    for other in (hop[0], hop[1], partner):
        pl.semaphore_signal(barrier, inc=1, device_id={"ep": other}, device_id_type=MESH_ID)
    pl.semaphore_wait(barrier, 3)

    def owner_at(way, dist, which):
        return member(-dist if way == RIGHT else dist, which)

    def part(ref, unit, way, dist):
        if dist == arm and unit != ROUTE:
            return ref.at[pl.ds(half * way, half)]
        return ref

    def present(unit, way, dist):
        return not (unit == ROUTE and dist == arm and way == LEFT)

    def send_on(unit, way, dist):
        if not present(unit, way, dist):
            return
        owner = owner_at(way, dist - 1, core)
        src = sources[unit] if dist == 1 else gathered[unit].at[owner]
        dst = gathered[unit].at[owner]
        launch(remote(part(src, unit, way, dist), part(dst, unit, way, dist),
                      ag_send.at[unit, way, dist - 1], ag_recv.at[unit, way, dist - 1], hop[way]))

    def await_ring(unit, way, dist):
        if not present(unit, way, dist):
            return
        ref = part(gathered[unit].at[owner_at(way, dist, core)], unit, way, dist)
        remote(ref, ref, ag_send.at[unit, way, dist - 1], ag_recv.at[unit, way, dist - 1], hop[way]).wait_recv()

    def send_over(unit, way, dist):
        if not present(unit, way, dist):
            return
        owner = owner_at(way, dist, core)
        src = sources[unit] if dist == 0 else gathered[unit].at[owner]
        launch(remote(part(src, unit, way, dist), part(gathered[unit].at[owner], unit, way, dist),
                      dd_send.at[unit, way, dist], dd_recv.at[unit, way, dist], partner))

    def await_over(unit, way, dist):
        if not present(unit, way, dist):
            return
        ref = part(gathered[unit].at[owner_at(way, dist, 1 - core)], unit, way, dist)
        remote(ref, ref, dd_send.at[unit, way, dist], dd_recv.at[unit, way, dist], partner).wait_recv()

    def begin(units):
        for unit in units:
            for way in (RIGHT, LEFT):
                send_on(unit, way, 1)
        for unit in units:
            send_over(unit, RIGHT, 0)

    def forward(units, dist):
        for unit in units:
            for way in (RIGHT, LEFT):
                await_ring(unit, way, dist)
                if dist < arm:
                    send_on(unit, way, dist + 1)
                send_over(unit, way, dist)

    spot = lax.broadcasted_iota(jnp.int32, (cap, tok), 0).astype(jnp.float32)
    earlier = (
        lax.broadcasted_iota(jnp.int32, (tok, tok), 0) < lax.broadcasted_iota(jnp.int32, (tok, tok), 1)
    ).astype(jnp.float32)

    def choose(owner):
        weights = rt_all[owner, me]
        chosen = (weights > 0.0).astype(jnp.float32)
        before = jnp.dot(chosen, earlier, preferred_element_type=jnp.float32)
        for kind in (FWD, BWD):
            hit = (spot == before[kind : kind + 1]) & (weights[kind : kind + 1] > 0.0)
            pick[kind, owner] = hit.astype(jnp.float32).astype(jnp.bfloat16)
            scale = jnp.sum(jnp.where(hit, weights[kind : kind + 1], 0.0), axis=1, keepdims=True)
            mixrow[kind, owner] = jnp.broadcast_to(scale, (cap, 128))

    def fetch(kind, owner, source, rows):
        rows[owner] = jnp.dot(
            pick[kind, owner], source[owner], preferred_element_type=jnp.float32
        ).astype(jnp.bfloat16)

    def take(kind, owner):
        if kind == BWD:
            choose(owner)
            fetch(BWD, owner, bt_all, xrows)
            fetch(BWD, owner, bg_all, grows)
        else:
            fetch(FWD, owner, ft_all, xrows)

    def take_ring(kind, dist):
        take(kind, owner_at(RIGHT, dist, core))
        if dist < arm:
            take(kind, owner_at(LEFT, dist, core))

    def take_over(kind, units, dist):
        ways = (RIGHT,) if dist == 0 else (RIGHT, LEFT)
        for unit in units:
            for way in ways:
                await_over(unit, way, dist)
        take(kind, owner_at(RIGHT, dist, 1 - core))
        if 0 < dist < arm:
            take(kind, owner_at(LEFT, dist, 1 - core))

    span = ep // 2

    def scaled(kind, first, value):
        scale = mixrow[kind, pl.ds(first, span)].reshape(span * cap, 128)[:, :1]
        zrows[kind, pl.ds(first, span)] = (value * scale).astype(jnp.bfloat16).reshape(span, cap, width)

    def nt(left, right):
        return lax.dot_general(left, right, (((1,), (1,)), ((), ())), preferred_element_type=jnp.float32)

    def expert_b(first):
        x = xrows[pl.ds(first, span)].reshape(span * cap, width)
        g = grows[pl.ds(first, span)].reshape(span * cap, width)
        p = jnp.dot(x, gate[...], preferred_element_type=jnp.float32)
        q = jnp.dot(x, up[...], preferred_element_type=jnp.float32)
        hidden_grad = nt(g, down[...])
        s = jax.nn.sigmoid(p)
        gate_grad = (hidden_grad * q * s * (1.0 + p * (1.0 - s))).astype(jnp.bfloat16)
        up_grad = (hidden_grad * p * s).astype(jnp.bfloat16)
        scaled(BWD, first, nt(gate_grad, gate[...]) + nt(up_grad, up[...]))

    def expert_f(first):
        x = xrows[pl.ds(first, span)].reshape(span * cap, width)
        p = jnp.dot(x, gate[...], preferred_element_type=jnp.float32)
        q = jnp.dot(x, up[...], preferred_element_type=jnp.float32)
        hidden = (p * jax.nn.sigmoid(p) * q).astype(jnp.bfloat16)
        scaled(FWD, first, jnp.dot(hidden, down[...], preferred_element_type=jnp.float32))

    def contribution(kind, owner):
        return lax.dot_general(
            pick[kind, owner], zrows[kind, owner], (((0,), (0,)), ((), ())), preferred_element_type=jnp.float32
        )

    order = [arm] + [j for d in range(arm - 1, 0, -1) for j in (d, ring - d)] + [0]

    def pair_copy(kind, j):
        return remote(pstage.at[kind, j], precv.at[kind, j], ps_send.at[kind, j], ps_recv.at[kind, j], partner)

    def hand_over(kind):
        for j in order:
            pstage[kind, j] = contribution(kind, member(j, 1 - core)).astype(jnp.bfloat16)
            launch(pair_copy(kind, j))

    def pair_sum(kind, j):
        pair_copy(kind, j).wait_recv()
        return contribution(kind, member(j, core)) + precv[kind, j].astype(jnp.float32)

    def ring_copy(kind, way, step):
        src, dst = rstage.at[kind, way, step], rrecv.at[kind, way, step]
        if step == 0:
            src, dst = src.at[pl.ds(half * way, half)], dst.at[pl.ds(half * way, half)]
        return remote(src, dst, rs_send.at[kind, way, step], rs_recv.at[kind, way, step], hop[way])

    def reduce_step(kind, step):
        dist = arm - step
        if step == 0:
            value = pair_sum(kind, arm).astype(jnp.bfloat16)
            for way in (RIGHT, LEFT):
                rows = pl.ds(half * way, half)
                rstage[kind, way, 0, rows] = value[half * way : half * way + half]
                launch(ring_copy(kind, way, 0))
            return
        for way in (RIGHT, LEFT):
            value = pair_sum(kind, dist if way == RIGHT else ring - dist)
            ring_copy(kind, way, step - 1).wait_recv()
            if step == 1:
                for at in (RIGHT, LEFT):
                    piece = value[half * at : half * at + half]
                    rows = pl.ds(half * at, half)
                    if at == way:
                        piece = piece + rrecv[kind, way, 0, rows].astype(jnp.float32)
                    rstage[kind, way, 1, rows] = piece.astype(jnp.bfloat16)
            else:
                rstage[kind, way, step] = (value + rrecv[kind, way, step - 1].astype(jnp.float32)).astype(
                    jnp.bfloat16
                )
            launch(ring_copy(kind, way, step))

    def finish(kind, out_ref):
        value = pair_sum(kind, 0)
        for way in (RIGHT, LEFT):
            ring_copy(kind, way, arm - 1).wait_recv()
            value = value + rrecv[kind, way, arm - 1].astype(jnp.float32)
        out_ref[...] = value.astype(jnp.bfloat16)

    units_b = (ROUTE, TOK_B, GRAD_B)
    units_f = (TOK_F,)
    begin(units_b)
    loads = [
        pltpu.make_async_copy(hbm.at[0], vmem, wsem.at[i])
        for i, (hbm, vmem) in enumerate(((gate_hbm, gate), (up_hbm, up), (down_hbm, down)))
    ]
    for load in loads:
        load.start()
    for unit in range(4):
        gathered[unit][me] = sources[unit][...]
    take(BWD, me)
    for dist in range(1, arm + 1):
        forward(units_b, dist)
        if dist == arm - 1:
            begin(units_f)
        if dist < arm:
            take_ring(BWD, dist)
        take_over(BWD, units_b, dist - 1)
    take_ring(BWD, arm)
    take_over(BWD, units_b, arm)
    for load in loads:
        load.wait()
    forward(units_f, 1)
    expert_b(0)
    if arm >= 2:
        forward(units_f, 2)
    expert_b(span)
    for dist in range(3, arm + 1):
        if dist < arm:
            forward(units_f, dist)
    hand_over(BWD)
    reduce_step(BWD, 0)
    if arm >= 3:
        forward(units_f, arm)
    take(FWD, me)
    for dist in range(1, arm):
        take_ring(FWD, dist)
    reduce_step(BWD, 1)
    take_ring(FWD, arm)
    for dist in range(0, arm + 1):
        take_over(FWD, units_f, dist)
    expert_f(0)
    for step in range(2, arm - 1):
        reduce_step(BWD, step)
    expert_f(span)
    if arm >= 3:
        reduce_step(BWD, arm - 1)
    hand_over(FWD)
    reduce_step(FWD, 0)
    finish(BWD, ob_ref)
    for step in range(1, arm):
        reduce_step(FWD, step)
    finish(FWD, of_ref)
    for copy in started:
        copy.wait_send()


def owner_weights(ids, mix, experts):
    named = ids[None, :, :] == jnp.arange(experts, dtype=jnp.int32)[:, None, None]
    return jnp.sum(jnp.where(named, mix[None, :, :], 0.0), axis=2)


def per_device_fused(
    forward_tokens,
    forward_ids,
    forward_mix,
    backward_tokens,
    backward_ids,
    backward_mix,
    backward_grad,
    gate_weight,
    up_weight,
    down_weight,
):
    tok, chosen = forward_ids.shape
    width = forward_tokens.shape[1]
    ep = lax.axis_size("ep")
    cap = tok * chosen * 4 // (3 * ep)
    ring = ep // 2
    arm = ring // 2
    bf16, f32 = jnp.bfloat16, jnp.float32
    route = jnp.stack(
        [owner_weights(forward_ids, forward_mix, ep), owner_weights(backward_ids, backward_mix, ep)], axis=1
    )
    vmem = pl.BlockSpec(memory_space=pltpu.VMEM)
    hbm = pl.BlockSpec(memory_space=pl.ANY)
    dma = pltpu.SemaphoreType.DMA
    return pl.pallas_call(
        functools.partial(fused_kernel, ep, cap),
        out_shape=(jax.ShapeDtypeStruct((tok, width), bf16),) * 2,
        in_specs=[vmem] * 4 + [hbm] * 3,
        out_specs=(vmem, vmem),
        scratch_shapes=[pltpu.VMEM((ep, tok, width), bf16)] * 3
        + [
            pltpu.VMEM((ep, ep, 2, tok), f32),
            pltpu.VMEM(gate_weight.shape[1:], bf16),
            pltpu.VMEM(up_weight.shape[1:], bf16),
            pltpu.VMEM(down_weight.shape[1:], bf16),
            pltpu.VMEM((2, ep, cap, tok), bf16),
            pltpu.VMEM((2, ep, cap, 128), f32),
            pltpu.VMEM((ep, cap, width), bf16),
            pltpu.VMEM((ep, cap, width), bf16),
            pltpu.VMEM((2, ep, cap, width), bf16),
            pltpu.VMEM((2, ring, tok, width), bf16),
            pltpu.VMEM((2, ring, tok, width), bf16),
            pltpu.VMEM((2, 2, arm, tok, width), bf16),
            pltpu.VMEM((2, 2, arm, tok, width), bf16),
            dma((3,)),
            dma((4, 2, arm)),
            dma((4, 2, arm)),
            dma((4, 2, arm + 1)),
            dma((4, 2, arm + 1)),
            dma((2, ring)),
            dma((2, ring)),
            dma((2, 2, arm)),
            dma((2, 2, arm)),
        ],
        compiler_params=pltpu.CompilerParams(
            collective_id=0, has_side_effects=True, vmem_limit_bytes=60 * 1024 * 1024
        ),
    )(forward_tokens, backward_tokens, backward_grad, route, gate_weight, up_weight, down_weight)


def fits_fused(mesh, tokens_shape, ids_shape):
    ep = mesh.shape["ep"]
    tok = tokens_shape[0] // (ep * mesh.shape["rep"])
    cap = tok * ids_shape[1] * 4 // (3 * ep)
    held = ep * tok * tokens_shape[1] * 2
    return ep % 4 == 0 and ep >= 12 and cap % 16 == 0 and 9 * held <= 36 * 1024 * 1024


def solution(mesh):
    rows = P(("rep", "ep"), None)
    stacked = P(("rep", "ep"), None, None)

    def run(*args):
        body = per_device_fused if fits_fused(mesh, args[0].shape, args[1].shape) else per_device
        return jax.shard_map(
            body, mesh=mesh, in_specs=(rows,) * 7 + (stacked,) * 3, out_specs=(rows, rows), check_vma=False
        )(*args)

    return run
```

```python
import functools

import jax
import jax.numpy as jnp
from jax import lax
from jax.experimental import pallas as pl
from jax.experimental.pallas import tpu as pltpu
from jax.sharding import PartitionSpec as P


def expert_forward(expert_rows, gate_matrix, up_matrix, down_matrix):
    gate_pre = jnp.dot(expert_rows, gate_matrix, preferred_element_type=jnp.float32)
    up_pre = jnp.dot(expert_rows, up_matrix, preferred_element_type=jnp.float32)
    hidden = (gate_pre * jax.nn.sigmoid(gate_pre) * up_pre).astype(jnp.bfloat16)
    return jnp.dot(hidden, down_matrix, preferred_element_type=jnp.float32).astype(jnp.bfloat16)


def expert_backward(expert_rows, row_grads, gate_matrix, up_matrix, down_matrix):
    gate_pre = jnp.dot(expert_rows, gate_matrix, preferred_element_type=jnp.float32)
    up_pre = jnp.dot(expert_rows, up_matrix, preferred_element_type=jnp.float32)
    sigmoid_gate = jax.nn.sigmoid(gate_pre)
    hidden_grad = jnp.dot(row_grads, down_matrix.T, preferred_element_type=jnp.float32)
    gate_grad = (
        hidden_grad * up_pre * sigmoid_gate * (1.0 + gate_pre * (1.0 - sigmoid_gate))
    ).astype(jnp.bfloat16)
    up_grad = (hidden_grad * gate_pre * sigmoid_gate).astype(jnp.bfloat16)
    rows_grad = jnp.dot(gate_grad, gate_matrix.T, preferred_element_type=jnp.float32)
    rows_grad = rows_grad + jnp.dot(up_grad, up_matrix.T, preferred_element_type=jnp.float32)
    return rows_grad.astype(jnp.bfloat16)


def route_targets(expert_ids, experts, capacity):
    tok_rows, chosen = expert_ids.shape
    flat_ids = expert_ids.reshape(tok_rows * chosen)
    onehot = (flat_ids[:, None] == jnp.arange(experts, dtype=jnp.int32)[None, :]).astype(jnp.int32)
    before = jnp.cumsum(onehot, axis=0) - onehot
    slot_index = jnp.sum(before * onehot, axis=1)
    return (flat_ids * capacity + slot_index).reshape(tok_rows, chosen)


def dispatch_rows(targets, experts, capacity, sources):
    places = jnp.arange(experts * capacity, dtype=jnp.int32)
    picker = jnp.any(targets[None, :, :] == places[:, None, None], axis=2).astype(jnp.bfloat16)
    return tuple(
        (
            jnp.dot(picker, values, preferred_element_type=jnp.float32)
            .astype(jnp.bfloat16)
            .reshape(experts, capacity, values.shape[1])
            for values in sources
        )
    )


def combine_rows(returned, targets, mixing):
    flat_rows = returned.reshape(returned.shape[0] * returned.shape[1], returned.shape[2])
    picked = flat_rows[targets].astype(jnp.float32)
    return jnp.sum(mixing[:, :, None] * picked, axis=1).astype(jnp.bfloat16)


def run_experts(received, apply, gate_weight, up_weight, down_weight):
    senders = lax.axis_size("ep")
    local_count = gate_weight.shape[0]
    slot_count = received[0].shape[1]
    feature_width = received[0].shape[2]
    expert_rows = tuple(
        (
            values.reshape(senders, local_count, slot_count, feature_width)[:, 0].reshape(
                senders * slot_count, feature_width
            )
            for values in received
        )
    )
    result = apply(expert_rows, gate_weight[0], up_weight[0], down_weight[0])
    outputs = [result.reshape(senders, slot_count, feature_width)]
    return jnp.stack(outputs, axis=1).reshape(senders * local_count, slot_count, feature_width)


def apply_forward(expert_rows, gate_matrix, up_matrix, down_matrix):
    return expert_forward(expert_rows[0], gate_matrix, up_matrix, down_matrix)


def apply_backward(expert_rows, gate_matrix, up_matrix, down_matrix):
    return expert_backward(expert_rows[0], expert_rows[1], gate_matrix, up_matrix, down_matrix)


def per_device(
    forward_tokens,
    forward_ids,
    forward_mix,
    backward_tokens,
    backward_ids,
    backward_mix,
    backward_grad,
    gate_weight,
    up_weight,
    down_weight,
):
    tok_rows, chosen = forward_ids.shape
    experts = lax.axis_size("ep") * gate_weight.shape[0]
    capacity = tok_rows * chosen * 4 // (3 * experts)
    targets_forward = route_targets(forward_ids, experts, capacity)
    targets_backward = route_targets(backward_ids, experts, capacity)
    (sent_forward,) = dispatch_rows(targets_forward, experts, capacity, (forward_tokens,))
    sent_backward, sent_grads = dispatch_rows(
        targets_backward, experts, capacity, (backward_tokens, backward_grad)
    )
    outputs_forward = run_experts(
        (lax.all_to_all(sent_forward, "ep", split_axis=0, concat_axis=0, tiled=True),),
        apply_forward,
        gate_weight,
        up_weight,
        down_weight,
    )
    back_forward = lax.all_to_all(outputs_forward, "ep", split_axis=0, concat_axis=0, tiled=True)
    outputs_backward = run_experts(
        (
            lax.all_to_all(sent_backward, "ep", split_axis=0, concat_axis=0, tiled=True),
            lax.all_to_all(sent_grads, "ep", split_axis=0, concat_axis=0, tiled=True),
        ),
        apply_backward,
        gate_weight,
        up_weight,
        down_weight,
    )
    back_backward = lax.all_to_all(outputs_backward, "ep", split_axis=0, concat_axis=0, tiled=True)
    forward_out = combine_rows(back_forward, targets_forward, forward_mix)
    input_grad = combine_rows(back_backward, targets_backward, backward_mix)
    return (forward_out, input_grad)


MESH_ID = pl.DeviceIdType.MESH
RIGHT, LEFT = 0, 1
TOK_B, GRAD_B, TOK_F, ROUTE = 0, 1, 2, 3
FWD, BWD = 0, 1


def fused_kernel(
    ep,
    cap,
    ft_ref,
    bt_ref,
    bg_ref,
    fi_ref,
    fm_ref,
    bi_ref,
    bm_ref,
    gate_hbm,
    up_hbm,
    down_hbm,
    of_ref,
    ob_ref,
    bt_all,
    bg_all,
    ft_all,
    rt_ref,
    rt_all,
    gate,
    up,
    down,
    pick,
    mixrow,
    xrows,
    grows,
    frows,
    zrows,
    pstage,
    precv,
    psum,
    rstage,
    rrecv,
    wsem,
    ag_send,
    ag_recv,
    dd_send,
    dd_recv,
    ps_send,
    ps_recv,
    rs_send,
    rs_recv,
):
    tok, width = ft_ref.shape
    half = tok // 2
    ring = ep // 2
    arm = ring // 2
    me = lax.axis_index("ep")
    core = lax.rem(me, 2)
    quo = me // 2
    row, col = quo // 2, lax.rem(quo, 2)
    pos = row + col * (ring - 1 - 2 * row)
    partner = me + 1 - 2 * core

    def member(offset, which):
        place = lax.rem(pos + offset + ring, ring)
        side = place // arm
        level = place + side * (ring - 1 - 2 * place)
        return 2 * (2 * level + side) + which

    hop = (member(1, core), member(-1, core))
    sources = (bt_ref, bg_ref, ft_ref, rt_ref)
    gathered = (bt_all, bg_all, ft_all, rt_all)
    started = []

    def remote(src, dst, send, recv, device):
        return pltpu.make_async_remote_copy(
            src_ref=src, dst_ref=dst, send_sem=send, recv_sem=recv,
            device_id={"ep": device}, device_id_type=MESH_ID,
        )

    def launch(copy):
        copy.start()
        started.append(copy)

    def table(ids_ref, mix_ref):
        named = lax.broadcasted_iota(jnp.int32, (ep, tok), 0)
        total = jnp.zeros((ep, tok), jnp.float32)
        for k in range(ids_ref.shape[0]):
            total = total + jnp.where(ids_ref[k : k + 1] == named, mix_ref[k : k + 1], 0.0)
        return total

    rt_ref[...] = jnp.concatenate([table(fi_ref, fm_ref), table(bi_ref, bm_ref)], axis=1)

    barrier = pltpu.get_barrier_semaphore()
    for other in (hop[0], hop[1], partner):
        pl.semaphore_signal(barrier, inc=1, device_id={"ep": other}, device_id_type=MESH_ID)
    pl.semaphore_wait(barrier, 3)

    def owner_at(way, dist, which):
        return member(-dist if way == RIGHT else dist, which)

    def part(ref, unit, way, dist):
        if dist == arm and unit != ROUTE:
            return ref.at[pl.ds(half * way, half)]
        return ref

    def present(unit, way, dist):
        return not (unit == ROUTE and dist == arm and way == LEFT)

    def send_on(unit, way, dist):
        if not present(unit, way, dist):
            return
        owner = owner_at(way, dist - 1, core)
        src = sources[unit] if dist == 1 else gathered[unit].at[owner]
        dst = gathered[unit].at[owner]
        launch(remote(part(src, unit, way, dist), part(dst, unit, way, dist),
                      ag_send.at[unit, way, dist - 1], ag_recv.at[unit, way, dist - 1], hop[way]))

    def await_ring(unit, way, dist):
        if not present(unit, way, dist):
            return
        ref = part(gathered[unit].at[owner_at(way, dist, core)], unit, way, dist)
        remote(ref, ref, ag_send.at[unit, way, dist - 1], ag_recv.at[unit, way, dist - 1], hop[way]).wait_recv()

    def send_over(unit, way, dist):
        if not present(unit, way, dist):
            return
        owner = owner_at(way, dist, core)
        src = sources[unit] if dist == 0 else gathered[unit].at[owner]
        launch(remote(part(src, unit, way, dist), part(gathered[unit].at[owner], unit, way, dist),
                      dd_send.at[unit, way, dist], dd_recv.at[unit, way, dist], partner))

    def await_over(unit, way, dist):
        if not present(unit, way, dist):
            return
        ref = part(gathered[unit].at[owner_at(way, dist, 1 - core)], unit, way, dist)
        remote(ref, ref, dd_send.at[unit, way, dist], dd_recv.at[unit, way, dist], partner).wait_recv()

    def begin(units):
        for unit in units:
            for way in (RIGHT, LEFT):
                send_on(unit, way, 1)
        for unit in units:
            send_over(unit, RIGHT, 0)

    def forward(units, dist):
        for unit in units:
            for way in (RIGHT, LEFT):
                await_ring(unit, way, dist)
                if dist < arm:
                    send_on(unit, way, dist + 1)
                send_over(unit, way, dist)

    spot = lax.broadcasted_iota(jnp.int32, (cap, tok), 0).astype(jnp.float32)
    first_at = lax.broadcasted_iota(jnp.int32, (2 * tok, 2 * tok), 0)
    then_at = lax.broadcasted_iota(jnp.int32, (2 * tok, 2 * tok), 1)
    earlier = ((first_at < then_at) & (first_at // tok == then_at // tok)).astype(jnp.float32)

    slots = {(RIGHT, 0, 0): 0}
    for dist in range(1, arm + 1):
        for same, reach in ((0, dist), (1, dist - 1)):
            for way in (RIGHT, LEFT):
                if 0 < reach < arm or way == RIGHT:
                    slots[way, reach, same] = len(slots)
    slots[RIGHT, arm, 1] = len(slots)

    def choose(owner, slot):
        weights = rt_all[owner, pl.ds(me, 1)]
        before = jnp.dot((weights > 0.0).astype(jnp.float32), earlier, preferred_element_type=jnp.float32)
        for kind in (FWD, BWD):
            lanes = slice(kind * tok, kind * tok + tok)
            hit = (spot == before[:, lanes]) & (weights[:, lanes] > 0.0)
            pick[kind, slot] = hit.astype(jnp.float32).astype(jnp.bfloat16)
            scale = jnp.sum(jnp.where(hit, weights[:, lanes], 0.0), axis=1, keepdims=True)
            mixrow[kind, slot] = jnp.broadcast_to(scale, (cap, 128))

    def fetch(kind, owner, slot, source, rows):
        rows[slot] = jnp.dot(
            pick[kind, slot], source[owner], preferred_element_type=jnp.float32
        ).astype(jnp.bfloat16)

    def take(kind, way, dist, same):
        slot = slots[way, dist, same]
        owner = owner_at(way, dist, core if same == 0 else 1 - core)
        if kind == BWD:
            choose(owner, slot)
            fetch(BWD, owner, slot, bt_all, xrows)
            fetch(BWD, owner, slot, bg_all, grows)
        else:
            fetch(FWD, owner, slot, ft_all, frows)

    def take_ring(kind, dist):
        take(kind, RIGHT, dist, 0)
        if 0 < dist < arm:
            take(kind, LEFT, dist, 0)

    def take_over(kind, units, dist):
        ways = (RIGHT,) if dist == 0 else (RIGHT, LEFT)
        for unit in units:
            for way in ways:
                await_over(unit, way, dist)
        take(kind, RIGHT, dist, 1)
        if 0 < dist < arm:
            take(kind, LEFT, dist, 1)

    def scaled(kind, first, span, value):
        scale = mixrow[kind, first : first + span].reshape(span * cap, 128)[:, :1]
        zrows[kind, first : first + span] = (value * scale).astype(jnp.bfloat16).reshape(span, cap, width)

    def nt(left, right):
        return lax.dot_general(left, right, (((1,), (1,)), ((), ())), preferred_element_type=jnp.float32)

    def nn(left, right):
        return jnp.dot(left, right, preferred_element_type=jnp.float32)

    def expert_b(first, span):
        x = xrows[first : first + span].reshape(span * cap, width)
        g = grows[first : first + span].reshape(span * cap, width)
        p = nt(x, gate[...])
        q = nt(x, up[...])
        hidden_grad = nt(g, down[...])
        s = jax.nn.sigmoid(p)
        gate_grad = (hidden_grad * q * s * (1.0 + p * (1.0 - s))).astype(jnp.bfloat16)
        up_grad = (hidden_grad * p * s).astype(jnp.bfloat16)
        scaled(BWD, first, span, nn(gate_grad, gate[...]) + nn(up_grad, up[...]))

    def expert_f(first, span):
        x = frows[first : first + span].reshape(span * cap, width)
        p = nt(x, gate[...])
        q = nt(x, up[...])
        hidden = (p * jax.nn.sigmoid(p) * q).astype(jnp.bfloat16)
        scaled(FWD, first, span, nn(hidden, down[...]))

    def contribution(kind, j, same):
        slot = slots[(RIGHT, ring - j, same) if j >= arm else (LEFT if j else RIGHT, j, same)]
        return lax.dot_general(
            pick[kind, slot], zrows[kind, slot], (((0,), (0,)), ((), ())), preferred_element_type=jnp.float32
        )

    order = [arm] + [j for d in range(arm - 1, 0, -1) for j in (d, ring - d)] + [0]

    def pair_copy(kind, j):
        return remote(pstage.at[kind, j], precv.at[kind, j], ps_send.at[kind, j], ps_recv.at[kind, j], partner)

    def hand_over(kind, places):
        for j in places:
            pstage[kind, j] = contribution(kind, j, 1).astype(jnp.bfloat16)
            launch(pair_copy(kind, j))

    def add_pair(kind, j):
        value = contribution(kind, j, 0)
        pair_copy(kind, j).wait_recv()
        psum[kind, j] = value + precv[kind, j].astype(jnp.float32)

    def ring_copy(kind, way, piece, dist):
        at = (kind, way, dist - 1, pl.ds(half * piece, half))
        return remote(rstage.at[at], rrecv.at[at], rs_send.at[kind, way, piece, dist - 1],
                      rs_recv.at[kind, way, piece, dist - 1], hop[way])

    def reach(way, piece):
        return arm if piece == way else arm - 1

    def pass_on(kind, way, piece, dist):
        rows = pl.ds(half * piece, half)
        value = psum[kind, dist if way == RIGHT else ring - dist, rows]
        if dist < reach(way, piece):
            ring_copy(kind, way, piece, dist + 1).wait_recv()
            value = value + rrecv[kind, way, dist, rows].astype(jnp.float32)
        rstage[kind, way, dist - 1, rows] = value.astype(jnp.bfloat16)
        launch(ring_copy(kind, way, piece, dist))

    def reduce_at(kind, dist):
        for lead in (True, False):
            for way in (RIGHT, LEFT):
                piece = way if lead else 1 - way
                if dist <= reach(way, piece):
                    pass_on(kind, way, piece, dist)

    def prepare(kind, dist):
        for j in (dist,) if dist in (0, arm) else (dist, ring - dist):
            add_pair(kind, j)

    def open_chains(kind):
        prepare(kind, arm)
        reduce_at(kind, arm)
        prepare(kind, arm - 1)
        for way in (RIGHT, LEFT):
            pass_on(kind, way, 1 - way, arm - 1)

    def second(kind):
        for way in (RIGHT, LEFT):
            pass_on(kind, way, way, arm - 1)

    def finish(kind, out_ref):
        for piece in (0, 1):
            rows = pl.ds(half * piece, half)
            value = psum[kind, 0, rows]
            for way in (RIGHT, LEFT):
                ring_copy(kind, way, piece, 1).wait_recv()
                value = value + rrecv[kind, way, 0, rows].astype(jnp.float32)
            out_ref[rows] = value.astype(jnp.bfloat16)

    units_b = (ROUTE, TOK_B, GRAD_B)
    units_f = (TOK_F,)
    begin(units_b)
    loads = [
        pltpu.make_async_copy(hbm.at[0], vmem, wsem.at[i])
        for i, (hbm, vmem) in enumerate(((gate_hbm, gate), (up_hbm, up), (down_hbm, down)))
    ]
    for load in loads:
        load.start()
    for unit in range(4):
        gathered[unit][me] = sources[unit][...]
    take(BWD, RIGHT, 0, 0)
    done = 0
    for dist in range(1, arm + 1):
        forward(units_b, dist)
        if dist == arm - 1:
            begin(units_f)
        take_ring(BWD, dist)
        take_over(BWD, units_b, dist - 1)
        if dist == 2:
            for load in loads:
                load.wait()
        if 2 <= dist < arm:
            ready = 4 * dist
            expert_b(done, ready - done)
            done = ready
    take_over(BWD, units_b, arm)
    forward(units_f, 1)
    expert_b(done, ep - done)
    hand_over(BWD, order[:3])
    take(FWD, RIGHT, 0, 0)
    take_ring(FWD, 1)
    take_over(FWD, units_f, 0)
    forward(units_f, 2)
    open_chains(BWD)
    hand_over(BWD, order[3:])
    take_ring(FWD, 2)
    take_over(FWD, units_f, 1)
    for dist in range(arm - 2, -1, -1):
        prepare(BWD, dist)
    forward(units_f, 3)
    second(BWD)
    expert_f(0, 8)
    done = 8
    for dist in range(4, arm + 1):
        take_ring(FWD, dist - 1)
        take_over(FWD, units_f, dist - 2)
        forward(units_f, dist)
        reduce_at(BWD, arm - dist + 2)
        expert_f(done, 4)
        done += 4
    take_ring(FWD, arm)
    take_over(FWD, units_f, arm - 1)
    take_over(FWD, units_f, arm)
    expert_f(done, ep - done)
    reduce_at(BWD, 1)
    hand_over(FWD, order[:3])
    open_chains(FWD)
    hand_over(FWD, order[3:])
    for dist in range(arm - 2, -1, -1):
        prepare(FWD, dist)
    second(FWD)
    finish(BWD, ob_ref)
    for dist in range(arm - 2, 0, -1):
        reduce_at(FWD, dist)
    finish(FWD, of_ref)
    for copy in started:
        copy.wait_send()


def settle_kernel(forward_ref, backward_ref, forward_out, backward_out):
    forward_out[...] = forward_ref[...]
    backward_out[...] = backward_ref[...]


def per_device_fused(
    forward_tokens,
    forward_ids,
    forward_mix,
    backward_tokens,
    backward_ids,
    backward_mix,
    backward_grad,
    gate_weight,
    up_weight,
    down_weight,
):
    tok, chosen = forward_ids.shape
    width = forward_tokens.shape[1]
    ep = lax.axis_size("ep")
    cap = tok * chosen * 4 // (3 * ep)
    ring = ep // 2
    arm = ring // 2
    bf16, f32 = jnp.bfloat16, jnp.float32
    vmem = pl.BlockSpec(memory_space=pltpu.VMEM)
    hbm = pl.BlockSpec(memory_space=pl.ANY)
    dma = pltpu.SemaphoreType.DMA
    results = pl.pallas_call(
        functools.partial(fused_kernel, ep, cap),
        out_shape=(jax.ShapeDtypeStruct((tok, width), bf16),) * 2,
        in_specs=[vmem] * 7 + [hbm] * 3,
        out_specs=(vmem, vmem),
        scratch_shapes=[pltpu.VMEM((ep, tok, width), bf16)] * 3
        + [
            pltpu.VMEM((ep, 2 * tok), f32),
            pltpu.VMEM((ep, ep, 2 * tok), f32),
            pltpu.VMEM(gate_weight.shape[:0:-1], bf16),
            pltpu.VMEM(up_weight.shape[:0:-1], bf16),
            pltpu.VMEM(down_weight.shape[1:], bf16),
            pltpu.VMEM((2, ep, cap, tok), bf16),
            pltpu.VMEM((2, ep, cap, 128), f32),
            pltpu.VMEM((ep, cap, width), bf16),
            pltpu.VMEM((ep, cap, width), bf16),
            pltpu.VMEM((ep, cap, width), bf16),
            pltpu.VMEM((2, ep, cap, width), bf16),
            pltpu.VMEM((2, ring, tok, width), bf16),
            pltpu.VMEM((2, ring, tok, width), bf16),
            pltpu.VMEM((2, ring, tok, width), f32),
            pltpu.VMEM((2, 2, arm, tok, width), bf16),
            pltpu.VMEM((2, 2, arm, tok, width), bf16),
            dma((3,)),
            dma((4, 2, arm)),
            dma((4, 2, arm)),
            dma((4, 2, arm + 1)),
            dma((4, 2, arm + 1)),
            dma((2, ring)),
            dma((2, ring)),
            dma((2, 2, 2, arm)),
            dma((2, 2, 2, arm)),
        ],
        compiler_params=pltpu.CompilerParams(
            collective_id=0, has_side_effects=True, vmem_limit_bytes=60 * 1024 * 1024
        ),
    )(
        forward_tokens,
        backward_tokens,
        backward_grad,
        forward_ids.T,
        forward_mix.T,
        backward_ids.T,
        backward_mix.T,
        gate_weight.swapaxes(1, 2),
        up_weight.swapaxes(1, 2),
        down_weight,
    )
    return tuple(
        pl.pallas_call(
            settle_kernel,
            out_shape=(jax.ShapeDtypeStruct((tok, width), bf16),) * 2,
            in_specs=[vmem] * 2,
            out_specs=(vmem, vmem),
        )(*results)
    )


def fits_fused(mesh, tokens_shape, ids_shape):
    ep = mesh.shape["ep"]
    tok = tokens_shape[0] // (ep * mesh.shape["rep"])
    cap = tok * ids_shape[1] * 4 // (3 * ep)
    held = ep * tok * tokens_shape[1] * 2
    return ep % 4 == 0 and ep >= 16 and cap % 16 == 0 and 11 * held <= 36 * 1024 * 1024


def solution(mesh):
    rows = P(("rep", "ep"), None)
    stacked = P(("rep", "ep"), None, None)

    def run(*args):
        body = per_device_fused if fits_fused(mesh, args[0].shape, args[1].shape) else per_device
        return jax.shard_map(
            body, mesh=mesh, in_specs=(rows,) * 7 + (stacked,) * 3, out_specs=(rows, rows), check_vma=False
        )(*args)

    return run
```
